32 devices in a mesh: bl: 8 (over z, x), tm: 4 (over y, core).
Axes of the slice: x: 2, y: 2, z: 4, core: 2. Of those that a mesh axis runs over, the one named last changes fastest.
Arguments:
- visibility_real: bfloat16 [3072, 16, 1024], P('bl', 'tm'), may hold values from -6 to 6
- visibility_imag: bfloat16 [3072, 16, 1024], P('bl', 'tm'), may hold values from -6 to 6
- weights: int32 [3072, 16], P('bl', 'tm'), may hold values from 0 to 8
- labels: int32 [3072], P('bl'), may hold values from 0 to 511, as said below
- owner_of: int32 [512], replicated, may hold values from 0 to 7, as said below
Outputs:
- bandpower: float32 [512, 1024], P(('bl', 'tm'))
The draws below stay inside these ranges and needn't reach their ends.
Inputs may be any that keep to these rules, and one draw needn't show every extreme that they name: Of the rows of one device, at most 72 have labels of groups with one owner, and these carry at most 18 different labels; in every draw some owner gets exactly 72 such rows with exactly 18 labels from every device. `owner_of`: every owner owns exactly 64 groups.
All inputs are finite; a program needn't handle non-finite values.
Results may differ from the reference program's by a relative error of at most 0.0003.
Values may be sent and summed in bfloat16 or wider, within the bound.
A program may use at most 128 MiB of HBM per device.

```python
import math
import jax
import jax.numpy as jnp
from jax import lax

FREQ_CHANNELS = 1024
B_DEV = 384
G_DEV = 64
BASELINE_COUNT = 3072
TIME_STEPS = 16
CAP = 72
KEYS = 18
N_BL = 8


def layout_plan(key):
    groups = G_DEV * N_BL
    group_order = jax.random.permutation(jax.random.fold_in(key, 101), groups).astype(jnp.int32)
    owner_of = jnp.zeros((groups,), jnp.int32).at[group_order].set(jnp.arange(groups, dtype=jnp.int32) // G_DEV)
    heaviest_owner = jax.random.randint(jax.random.fold_in(key, 102), (), 0, N_BL)

    def one_device(device):
        device_key = jax.random.fold_in(jax.random.fold_in(key, 103), device)
        slot_ids = jnp.arange(N_BL * CAP, dtype=jnp.int32)
        priority = jax.random.permutation(jax.random.fold_in(device_key, 1), N_BL * CAP).astype(jnp.int32)
        priority = jnp.where(slot_ids // CAP == heaviest_owner, priority - N_BL * CAP, priority)
        chosen = jnp.argsort(priority)[:B_DEV].astype(jnp.int32)
        target = chosen // CAP
        within = chosen % CAP

        def candidates(owner):
            owner_key = jax.random.fold_in(jax.random.fold_in(device_key, 2), owner)
            return jax.random.permutation(owner_key, G_DEV)[:KEYS].astype(jnp.int32)
        offsets = jax.vmap(candidates)(jnp.arange(N_BL, dtype=jnp.int32))
        picked = offsets[target, within % KEYS]
        row_label = group_order[target * G_DEV + picked]
        shuffle = jax.random.permutation(jax.random.fold_in(device_key, 3), B_DEV)
        return row_label[shuffle]
    labels = jax.vmap(one_device)(jnp.arange(N_BL, dtype=jnp.int32)).reshape(-1)
    return (labels.astype(jnp.int32), owner_of)


def draw_labels(key, part):
    return layout_plan(key)[0]


def draw_owner_of(key, part):
    return layout_plan(key)[1]


def set_ends(values, stream_key, low, top_value):
    dims = values.shape
    index_at = [jax.random.randint(jax.random.fold_in(stream_key, axis), (), 0, dims[axis]) for axis in range(len(dims))]
    values = values.at[tuple(index_at)].set(low)
    longest = dims.index(max(dims))
    index_at[longest] = (index_at[longest] + 1) % dims[longest]
    return values.at[tuple(index_at)].set(top_value)


def shard_levels(key, dims, split, smallest, largest):
    loudness = 1.0
    for dim, blocks in split:
        draws = jax.random.uniform(jax.random.fold_in(jax.random.fold_in(key, 6), dim), (blocks,), jnp.float32, smallest / len(split), largest / len(split))
        loudness = loudness * jnp.repeat(jnp.exp(draws), dims[dim] // blocks).reshape((-1,) + (1,) * (len(dims) - 1 - dim))
    return loudness


def noise(key, shape, width, reach, shards=(), kind=jnp.bfloat16):
    level = shard_levels(key, shape, shards, -0.22, 0.18) if shards else 1.0
    array = jax.random.normal(key, shape, jnp.float32) * width * level
    return jnp.minimum(jnp.maximum(array, -reach), reach).astype(kind)


def setup_inputs(seed: int = 0) -> dict:
    keys = jax.random.split(jax.random.key(seed), 6)
    return {
        "visibility_real": noise(keys[0], (BASELINE_COUNT, TIME_STEPS, FREQ_CHANNELS), 1.0, 6.0, ((0, 8), (1, 4))),
        "visibility_imag": noise(keys[1], (BASELINE_COUNT, TIME_STEPS, FREQ_CHANNELS), 1.0, 6.0, ((0, 8), (1, 4))),
        "weights": set_ends(jax.random.randint(keys[2], (BASELINE_COUNT, TIME_STEPS), 0, 9), jax.random.fold_in(keys[2], 1), 0, 8).astype(jnp.int32),
        "labels": draw_labels(jax.random.fold_in(keys[5], 71), 0),
        "owner_of": draw_owner_of(jax.random.fold_in(keys[5], 71), 0),
    }


HARRIS = (0.35875, 0.48829, 0.14128, 0.01168)

def taper_of(length):
    phase_angle = 2.0 * math.pi / length * jnp.arange(length, dtype=jnp.float32)
    return HARRIS[0] - HARRIS[1] * jnp.cos(phase_angle) + HARRIS[2] * jnp.cos(2.0 * phase_angle) - HARRIS[3] * jnp.cos(3.0 * phase_angle)

def reference(visibility_real, visibility_imag, weights, labels, owner_of):
    groups = owner_of.shape[0]
    channels = visibility_real.shape[2]
    times = visibility_real.shape[1]
    window_taper = taper_of(channels)
    window_taper = window_taper / jnp.sqrt(jnp.sum(window_taper * window_taper))

    def advance(carried, instant):
        prior_real, prior_imag, running = carried
        row_weight = lax.dynamic_index_in_dim(weights, instant, 1, keepdims=False).astype(jnp.float32)
        slab_real = lax.dynamic_index_in_dim(visibility_real, instant, 1, keepdims=False).astype(jnp.float32)
        slab_imag = lax.dynamic_index_in_dim(visibility_imag, instant, 1, keepdims=False).astype(jnp.float32)
        sum_real = jax.ops.segment_sum(row_weight[:, None] * slab_real, labels, num_segments=groups)
        sum_imag = jax.ops.segment_sum(row_weight[:, None] * slab_imag, labels, num_segments=groups)
        weight_sum = jax.ops.segment_sum(row_weight, labels, num_segments=groups)
        divisor = jnp.maximum(weight_sum, 1.0)[:, None]
        mean_real = sum_real / divisor
        mean_imag = sum_imag / divisor
        spectrum = jnp.fft.fft((mean_real + 1j * mean_imag) * window_taper[None, :], axis=1)
        spec_real = jnp.real(spectrum)
        spec_imag = jnp.imag(spectrum)
        cross = prior_real * spec_real + prior_imag * spec_imag
        running = running + jnp.where(instant > 0, cross, jnp.zeros_like(cross))
        return ((spec_real, spec_imag, running), instant)
    zeros = jnp.zeros((groups, channels), jnp.float32)
    final_state, unused = lax.scan(advance, (zeros, zeros, zeros), jnp.arange(times, dtype=jnp.int32))
    order = jnp.argsort(owner_of * groups + jnp.arange(groups, dtype=jnp.int32))
    return final_state[2][order]
```

```python
import functools
import math

import jax
import jax.numpy as jnp
from jax import lax
from jax.experimental import pallas as pl
from jax.experimental.pallas import tpu as pltpu
from jax.sharding import PartitionSpec as P

HARRIS = (0.35875, 0.48829, 0.14128, 0.01168)
RADIX = 4
F32, BF16, I32 = jnp.float32, jnp.bfloat16, jnp.int32
MESH = pl.DeviceIdType.MESH


def iota(shape, dim):
    return lax.broadcasted_iota(I32, shape, dim)


def dot(a, b):
    return jnp.dot(a, b, preferred_element_type=F32)


def halves(value):
    high = value.astype(BF16)
    return high, (value - high.astype(F32)).astype(BF16)


def lanes(count):
    return -(-max(count, 1) // 128) * 128


def partner(me, step, size):
    if size & (size - 1):
        return lax.rem(me + step, size)
    peer, bit = 0, 1
    while bit < size:
        mine = lax.rem(me // bit, 2)
        peer = peer + bit * (1 - mine if step & bit else mine)
        bit *= 2
    return peer


class Plan:
    def __init__(self, row_count, times, channels, groups, owners, parts):
        capacity = 3 * row_count // (2 * owners)
        self.rows, self.times, self.channels, self.groups = row_count, times, channels, groups
        self.owners, self.parts = owners, parts
        self.per_owner = groups // owners
        self.distinct = min(capacity // 4, self.per_owner // 2)
        self.main = self.distinct // 8 * 8
        self.extra = self.distinct - self.main
        self.tail = -(-self.extra * times // 8) * 8
        self.mains = owners * self.main
        self.tails = owners * self.tail
        self.wide = max(lanes(self.mains), lanes(self.tails))
        self.facts = -(-(times + 4) // 8) * 8


def program_kernel(
    plan, vis_real, vis_imag, weights, labels, owner_of, out,
    fresh, part, part_tail, send, send_tail, send_note, send_step,
    came, came_tail, came_note, came_step,
    table, taper, total, spectrum, following, share, shared,
    loads, sends, arrivals, tail_sends, tail_arrivals,
):
    p = plan
    T, N, F, G, R = p.times, p.owners, p.channels, p.groups, p.rows
    pairs, both = T // 2, 2 * R
    short = F // RADIX
    me = lax.axis_index("bl")
    here = lax.axis_index("tm")

    incoming = []
    for pair in range(pairs):
        for which, source in enumerate((vis_real, vis_imag)):
            copy = pltpu.make_async_copy(
                source.at[:, pl.ds(2 * pair, 2)], fresh.at[pair, which], loads.at[pair, which]
            )
            copy.start()
            incoming.append(copy)

    barrier = pltpu.get_barrier_semaphore()
    for hop in range(1, N):
        pl.semaphore_signal(
            barrier, inc=1, device_id={"bl": lax.rem(me + hop, N)}, device_id_type=MESH
        )
    for hop in range(1, p.parts):
        pl.semaphore_signal(
            barrier, inc=1, device_id={"tm": lax.rem(here + hop, p.parts)}, device_id_type=MESH
        )

    label = labels[...]
    base = jnp.concatenate(
        [
            (label // 256).astype(F32),
            lax.rem(label, 256).astype(F32),
            weights[...].astype(F32),
            jnp.zeros((-(T + 2) % 8, R), F32),
        ],
        axis=0,
    )
    spread = (iota((R, both), 1) // 2 == iota((R, both), 0)).astype(F32).astype(BF16)
    doubled = dot(base.astype(BF16), spread)
    label_twice = (doubled[0:1] * 256.0 + doubled[1:2]).astype(I32)
    hit = (iota((G, both), 0) == label_twice).astype(F32).astype(BF16)
    count = lax.dot_general(
        jnp.ones((8, both), BF16), hit, (((1,), (1,)), ((), ())), preferred_element_type=F32
    )
    present = (count[0:1] > 0.5).astype(F32)
    owner = owner_of[...]
    owned = (iota((N, G), 0) == owner).astype(F32)
    before = (iota((G, G), 0) < iota((G, G), 1)).astype(F32).astype(BF16)
    earlier = dot(jnp.concatenate([owned, owned * present], axis=0).astype(BF16), before)
    rank = jnp.sum(owned * earlier[:N], axis=0, keepdims=True)
    order = jnp.sum(owned * earlier[N:], axis=0, keepdims=True)
    info = jnp.concatenate([owner.astype(F32), order, jnp.zeros((6, G), F32)], axis=0)
    placed = dot(info.astype(BF16), hit)
    row_owner = placed[0:1].astype(I32)
    row_order = placed[1:2].astype(I32)
    second = lax.rem(iota((1, both), 1), 2)

    listed = order.astype(I32)
    seen = present > 0.5
    rank_main = rank_tail = None
    if p.main:
        slot_main = jnp.where(seen & (listed < p.main), owner * p.main + listed, -1)
        rank_main = jnp.sum(
            jnp.where(iota((p.mains, G), 0) == slot_main, rank, 0.0), axis=1, keepdims=True
        )
    if p.extra:
        slot_tail = jnp.where(
            seen & (listed >= p.main), owner * p.extra + listed - p.main, -1
        )
        row = iota((p.tails, 1), 0)
        within = lax.rem(row, p.tail)
        slot_of_row = row // p.tail * p.extra + lax.rem(within, p.extra)
        rank_tail = jnp.sum(
            jnp.where((slot_of_row == slot_tail) & (within < p.extra * T), rank, 0.0),
            axis=1,
            keepdims=True,
        )

    def laid(column, height):
        block = jnp.broadcast_to(column, (column.shape[0], p.wide))
        shape = block.shape
        match = lax.rem(iota(shape, 0), height) == lax.rem(iota(shape, 1), height)
        block = jnp.where(match, block, 0.0).reshape(shape[0] // height, height, p.wide)
        return jnp.sum(block, axis=1, keepdims=True)

    send_note[...] = jnp.zeros_like(send_note)
    if p.main:
        send_note[:, 0:1] = laid(rank_main, p.main)
    if p.extra:
        send_note[:, T + 1 : T + 2] = laid(rank_tail, p.tail)

    def start(kind, peer):
        if kind < T:
            pieces = [(send.at[kind], came.at[kind], kind)]
            pieces.append((send_step.at[kind], came_step.at[kind], T + kind))
        else:
            pieces = [(send_note, came_note, 2 * T + 1)]
            if p.extra:
                pieces.append((send_tail, came_tail, 2 * T))
        return [
            pltpu.make_async_remote_copy(
                src_ref=source.at[peer],
                dst_ref=target.at[me],
                send_sem=sends.at[index, peer],
                recv_sem=arrivals.at[index, me],
                device_id={"bl": peer},
                device_id_type=MESH,
            )
            for source, target, index in pieces
        ]

    def arrive(kind, source):
        if kind < T:
            pieces = [(send.at[kind], came.at[kind], kind)]
            pieces.append((send_step.at[kind], came_step.at[kind], T + kind))
        else:
            pieces = [(send_note, came_note, 2 * T + 1)]
            if p.extra:
                pieces.append((send_tail, came_tail, 2 * T))
        return [
            pltpu.make_async_remote_copy(
                src_ref=origin.at[source],
                dst_ref=target.at[source],
                send_sem=sends.at[index, source],
                recv_sem=arrivals.at[index, source],
                device_id={"bl": source},
                device_id_type=MESH,
            )
            for origin, target, index in pieces
        ]

    def post(kind):
        for step in range(1, N):
            for copy in start(kind, partner(me, step, N)):
                copy.start()

    def encode(real, imag):
        peak = jnp.maximum(
            jnp.max(jnp.abs(real), axis=1, keepdims=True),
            jnp.max(jnp.abs(imag), axis=1, keepdims=True),
        )
        step = jnp.maximum(peak, 1e-30) * (1.0078125 / 32767.0)
        step = step.astype(BF16).astype(F32)
        invert = 1.0 / step
        code_real = jnp.round(real * invert).astype(I32)
        code_imag = jnp.round(imag * invert).astype(I32)
        return (code_real << 16) | (code_imag & 65535), step

    def encode_main(time):
        offset = time % 2 * p.mains

        def one(o, carry):
            at = pl.multiple_of(offset + o * p.main, 8)
            code, step = encode(part[0, pl.ds(at, p.main)], part[1, pl.ds(at, p.main)])
            send[time, o] = code
            send_step[time, o] = laid(step, p.main)[0]
            return carry

        lax.fori_loop(0, N, one, 0)
        came[time, me] = send[time, me]
        came_step[time, me] = send_step[time, me]

    def encode_tail():
        def one(o, carry):
            at = pl.multiple_of(o * p.tail, 8)
            code, step = encode(part_tail[0, pl.ds(at, p.tail)], part_tail[1, pl.ds(at, p.tail)])
            send_tail[o] = code
            send_note[o, T + 3 : T + 4] = laid(step, p.tail)[0]
            return carry

        lax.fori_loop(0, N, one, 0)
        came_tail[me] = send_tail[me]

    all_rows = 2 * p.mains + p.tails
    tail_weight = jnp.zeros((p.tails, 1), F32)
    for pair in range(pairs):
        weight = jnp.where(
            second == 0, doubled[2 + 2 * pair : 3 + 2 * pair], doubled[3 + 2 * pair : 4 + 2 * pair]
        )
        target = jnp.where(
            row_order < p.main,
            second * p.mains + row_owner * p.main + row_order,
            2 * p.mains
            + row_owner * p.tail
            + (2 * pair + second) * p.extra
            + row_order
            - p.main,
        )
        folder = jnp.where(iota((all_rows, both), 0) == target, weight, 0.0)
        sums = jnp.sum(folder, axis=1, keepdims=True)
        folder = folder.astype(BF16)
        for copy in incoming[2 * pair : 2 * pair + 2]:
            copy.wait()
        for which in range(2):
            made = dot(folder, fresh[pair, which].reshape(both, F))
            if p.main:
                part[which] = made[: 2 * p.mains]
            if p.extra:
                if pair:
                    part_tail[which] += made[2 * p.mains :]
                else:
                    part_tail[which] = made[2 * p.mains :]
        if p.main:
            send_note[:, 1 + 2 * pair : 2 + 2 * pair] = laid(sums[: p.mains], p.main)
            send_note[:, 2 + 2 * pair : 3 + 2 * pair] = laid(sums[p.mains : 2 * p.mains], p.main)
        if p.extra:
            tail_weight = tail_weight + sums[2 * p.mains :]
        if pair == 0:
            if p.main:
                encode_main(0)
            pl.semaphore_wait(barrier, N + p.parts - 2)
            if p.main:
                post(0)
                encode_main(1)
                if pairs == 1:
                    post(1)
        if pair == pairs - 1:
            if p.extra:
                send_note[:, T + 2 : T + 3] = laid(tail_weight, p.tail)
                encode_tail()
            came_note[me] = send_note[me]
            post(T)
            if p.main and pairs > 1:
                post(1)
        if p.main and pair:
            for time in (2 * pair, 2 * pair + 1):
                encode_main(time)
                post(time)

    turn = 2.0 * math.pi / F
    phase = turn * iota((1, F), 1).astype(F32)
    shape = (
        HARRIS[0]
        - HARRIS[1] * jnp.cos(phase)
        + HARRIS[2] * jnp.cos(2.0 * phase)
        - HARRIS[3] * jnp.cos(3.0 * phase)
    )
    taper[...] = shape / jnp.sqrt(jnp.sum(shape * shape, axis=1, keepdims=True))
    fine = 16
    for q in range(RADIX):
        delay = RADIX * iota((fine, short), 1) + q
        low = turn * lax.rem(iota((fine, short), 0) * delay, F).astype(F32)
        high = turn * lax.rem(fine * iota((fine, short), 0) * delay, F).astype(F32)
        low_cos, low_sin = jnp.cos(low), jnp.sin(low)
        high_cos, high_sin = jnp.cos(high), jnp.sin(high)
        for a in range(short // fine):
            ac, as_ = high_cos[a : a + 1], high_sin[a : a + 1]
            rows = pl.ds(a * fine, fine)
            upper, lower = halves(ac * low_cos - as_ * low_sin)
            table[q, 0, rows, :short] = upper
            table[q, 1, rows, :short] = lower
            upper, lower = halves(as_ * low_cos + ac * low_sin)
            table[q, 0, rows, short:] = upper
            table[q, 1, rows, short:] = lower

    def wait_for(kind):
        for step in range(1, N):
            for copy in arrive(kind, partner(me, step, N)):
                copy.wait_recv()

    def planes(code):
        real_high = (code >> 24).astype(F32).astype(BF16)
        real_low = ((code >> 16) & 255).astype(F32).astype(BF16)
        imag = (code << 16) >> 16
        imag_high = (imag >> 8).astype(F32).astype(BF16)
        imag_low = (imag & 255).astype(F32).astype(BF16)
        return (
            jnp.concatenate([real_high, real_low], axis=0),
            jnp.concatenate([imag_high, imag_low], axis=0),
        )

    def gathered(values, height):
        shape = values.shape
        mine = iota(shape, 2) // height == iota(shape, 0)
        return jnp.sum(jnp.where(mine, values, 0.0), axis=0)

    wait_for(T)
    facts = came_note[...]
    rank_row = iota((p.per_owner, 1), 0).astype(F32)
    chosen_main = facts_main = None
    if p.main:
        facts_main = gathered(facts, p.main)[:, : p.mains]
        chosen_main = rank_row == facts_main[0:1]
    tail_sums = []
    if p.extra:
        facts_tail = gathered(facts, p.tail)[:, : p.tails]
        tail_real, tail_imag = planes(came_tail[...].reshape(p.tails, F))
        lane = lax.rem(iota((1, p.tails), 1), p.tail)
        lane_time = jnp.where(lane < p.extra * T, lane // p.extra, T)
        selectors = []
        for time in range(T):
            chosen = (rank_row == facts_tail[T + 1 : T + 2]) & (lane_time == time)
            selector = jnp.where(chosen, facts_tail[T + 3 : T + 4], 0.0)
            selectors.append(jnp.concatenate([256.0 * selector, selector], axis=1))
            tail_sums.append(
                jnp.sum(
                    jnp.where(chosen, facts_tail[T + 2 : T + 3], 0.0), axis=1, keepdims=True
                )
            )
        selectors = jnp.concatenate(selectors, axis=0).astype(BF16)
        total[0] = dot(selectors, tail_real)
        total[1] = dot(selectors, tail_imag)
    for time in range(T):
        weight_sum = jnp.zeros((p.per_owner, 1), F32)
        if p.extra:
            weight_sum = weight_sum + tail_sums[time]
        block = pl.ds(time * p.per_owner, p.per_owner)
        real = imag = 0.0
        if p.extra:
            real, imag = total[0, block], total[1, block]
        if p.main:
            wait_for(time)
            steps = gathered(came_step[time], p.main)[:, : p.mains]
            selector = jnp.where(chosen_main, steps, 0.0)
            selector = jnp.concatenate([256.0 * selector, selector], axis=1).astype(BF16)
            weight_sum = weight_sum + jnp.sum(
                jnp.where(chosen_main, facts_main[1 + time : 2 + time], 0.0),
                axis=1,
                keepdims=True,
            )
            main_real, main_imag = planes(came[time].reshape(p.mains, F))
            real = real + dot(selector, main_real)
            imag = imag + dot(selector, main_imag)
        scale = 1.0 / jnp.maximum(weight_sum, 1.0)
        window = taper[...]
        real = real * scale * window
        imag = imag * scale * window
        r = [real[:, i * short : (i + 1) * short] for i in range(RADIX)]
        m = [imag[:, i * short : (i + 1) * short] for i in range(RADIX)]
        er, ei, fr, fi = r[0] + r[2], m[0] + m[2], r[1] + r[3], m[1] + m[3]
        gr, gi, hr, hi = r[0] - r[2], m[0] - m[2], r[1] - r[3], m[1] - m[3]
        folded = (
            (er + fr, ei + fi),
            (gr + hi, gi - hr),
            (er - fr, ei - fi),
            (gr - hi, gi + hr),
        )
        n = p.per_owner
        for q in range(RADIX):
            stacked = jnp.concatenate(folded[q], axis=0)
            upper, lower = halves(stacked)
            first = dot(jnp.concatenate([upper, lower], axis=0), table[q, 0])
            wave = first[: 2 * n] + first[2 * n :] + dot(upper, table[q, 1])
            spectrum[time, q, :, :short] = wave[:n, :short] + wave[n:, short:]
            spectrum[time, q, :, short:] = wave[n:, :short] - wave[:n, short:]
        if time == 0:
            ahead = pltpu.make_async_remote_copy(
                src_ref=spectrum.at[0],
                dst_ref=following,
                send_sem=tail_sends.at[p.parts - 1],
                recv_sem=tail_arrivals.at[p.parts - 1],
                device_id={"tm": lax.rem(here + p.parts - 1, p.parts)},
                device_id_type=MESH,
            )
            ahead.start()
        else:
            for q in range(RADIX):
                product = spectrum[time - 1, q] * spectrum[time, q]
                power = product[:, :short] + product[:, short:]
                power = power.reshape(p.parts, n // p.parts, short)
                if time == 1:
                    share[:, q] = power
                else:
                    share[:, q] += power
    ahead.wait()
    for q in range(RADIX):
        product = spectrum[T - 1, q] * following[q]
        power = product[:, :short] + product[:, short:]
        power = jnp.where(here < p.parts - 1, power, 0.0)
        share[:, q] += power.reshape(p.parts, p.per_owner // p.parts, short)
    copies = []
    for hop in range(1, p.parts):
        peer = lax.rem(here + hop, p.parts)
        copy = pltpu.make_async_remote_copy(
            src_ref=share.at[peer],
            dst_ref=shared.at[hop - 1],
            send_sem=tail_sends.at[hop - 1],
            recv_sem=tail_arrivals.at[hop - 1],
            device_id={"tm": peer},
            device_id_type=MESH,
        )
        copy.start()
        copies.append(copy)
    summed = share[here]
    for kind in range(T + 1):
        if kind == T or p.main:
            for step in range(1, N):
                for copy in start(kind, partner(me, step, N)):
                    copy.wait_send()
    for hop, copy in enumerate(copies):
        copy.wait()
        summed = summed + shared[hop]
    rows = p.per_owner // p.parts
    lane = iota((rows, 128), 1)
    for tile in range(F // 128):
        begin = tile * 128 // RADIX
        block = begin // 128 * 128
        index = lane // RADIX + (begin - block)
        value = None
        for q in range(RADIX):
            picked = jnp.take_along_axis(summed[q, :, block : block + 128], index, axis=1)
            value = picked if value is None else jnp.where(lax.rem(lane, RADIX) == q, picked, value)
        out[:, tile * 128 : (tile + 1) * 128] = value


def per_device(visibility_real, visibility_imag, weights, labels, owner_of):
    row_count, times, channels = visibility_real.shape
    owners, parts = lax.axis_size("bl"), lax.axis_size("tm")
    p = Plan(row_count, times, channels, owner_of.shape[0], owners, parts)
    short = channels // RADIX
    inside = pl.BlockSpec(memory_space=pltpu.VMEM)
    outside = pl.BlockSpec(memory_space=pltpu.HBM)
    some = lambda count: max(count, 8)
    main, tail = some(p.main), some(p.tail)
    rows = p.per_owner // parts
    return pl.pallas_call(
        functools.partial(program_kernel, p),
        out_shape=jax.ShapeDtypeStruct((rows, channels), F32),
        in_specs=[outside, outside, inside, inside, inside],
        out_specs=inside,
        scratch_shapes=[
            pltpu.VMEM((times // 2, 2, row_count, 2, channels), BF16),
            pltpu.VMEM((2, some(2 * p.mains), channels), F32),
            pltpu.VMEM((2, some(p.tails), channels), F32),
            pltpu.VMEM((times, owners, main, channels), I32),
            pltpu.VMEM((owners, tail, channels), I32),
            pltpu.VMEM((owners, p.facts, p.wide), F32),
            pltpu.VMEM((times, owners, 1, p.wide), F32),
            pltpu.VMEM((times, owners, main, channels), I32),
            pltpu.VMEM((owners, tail, channels), I32),
            pltpu.VMEM((owners, p.facts, p.wide), F32),
            pltpu.VMEM((times, owners, 1, p.wide), F32),
            pltpu.VMEM((RADIX, 2, short, 2 * short), BF16),
            pltpu.VMEM((1, channels), F32),
            pltpu.VMEM((2, times * p.per_owner, channels), F32),
            pltpu.VMEM((times, RADIX, p.per_owner, 2 * short), F32),
            pltpu.VMEM((RADIX, p.per_owner, 2 * short), F32),
            pltpu.VMEM((parts, RADIX, rows, short), F32),
            pltpu.VMEM((parts - 1, RADIX, rows, short), F32),
            pltpu.SemaphoreType.DMA((times // 2, 2)),
            pltpu.SemaphoreType.DMA((2 * times + 2, owners)),
            pltpu.SemaphoreType.DMA((2 * times + 2, owners)),
            pltpu.SemaphoreType.DMA((parts,)),
            pltpu.SemaphoreType.DMA((parts,)),
        ],
        compiler_params=pltpu.CompilerParams(
            collective_id=0, has_side_effects=True, vmem_limit_bytes=60 * 2**20
        ),
    )(visibility_real, visibility_imag, weights.T, labels[None, :], owner_of[None, :])


def solution(mesh):
    placed = (P("bl", "tm", None), P("bl", "tm", None), P("bl", "tm"), P("bl"), P())
    return jax.shard_map(
        per_device, mesh=mesh, in_specs=placed, out_specs=P(("bl", "tm"), None), check_vma=False
    )
```

```python
import functools
import math

import jax
import jax.numpy as jnp
from jax import lax
from jax.experimental import pallas as pl
from jax.experimental.pallas import tpu as pltpu
from jax.sharding import PartitionSpec as P

HARRIS = (0.35875, 0.48829, 0.14128, 0.01168)
RADIX = 4
F32, BF16, I32 = jnp.float32, jnp.bfloat16, jnp.int32
MESH = pl.DeviceIdType.MESH


def iota(shape, dim):
    return lax.broadcasted_iota(I32, shape, dim)


def dot(a, b):
    return jnp.dot(a, b, preferred_element_type=F32)


def halves(value):
    high = value.astype(BF16)
    return high, (value - high.astype(F32)).astype(BF16)


def lanes(count):
    return -(-max(count, 1) // 128) * 128


def partner(me, step, size):
    if size & (size - 1):
        return lax.rem(me + step, size)
    peer, bit = 0, 1
    while bit < size:
        peer = peer + bit * lax.rem(lax.rem(me // bit, 2) + step // bit, 2)
        bit *= 2
    return peer


class Plan:
    def __init__(self, row_count, times, channels, groups, owners, parts):
        capacity = 3 * row_count // (2 * owners)
        self.rows, self.times, self.channels, self.groups = row_count, times, channels, groups
        self.owners, self.parts = owners, parts
        self.per_owner = groups // owners
        self.distinct = min(capacity // 4, self.per_owner // 2)
        self.main = self.distinct // 16 * 16
        self.extra = self.distinct - self.main
        self.tail = -(-self.extra * times // 8) * 8
        self.mains = owners * self.main
        self.tails = owners * self.tail
        assert times * self.main + 2 * self.tail <= 128


def program_kernel(
    plan, vis_real, vis_imag, weights, labels, owner_of, out,
    weight_in, label_in, owner_in,
    fresh, part, part_tail, send, send_tail, send_note, send_step,
    came, came_tail, came_note, came_step,
    table, taper, total, planes, spectrum, following, share, shared,
    loads, small, sends, arrivals, ahead_sems, tail_sends, tail_arrivals,
):
    p = plan
    T, N, F, G, R = p.times, p.owners, p.channels, p.groups, p.rows
    pairs, both = T // 2, 2 * R
    short = F // RADIX
    n = p.per_owner
    me = lax.axis_index("bl")
    here = lax.axis_index("tm")

    inputs = [
        pltpu.make_async_copy(source, target, small.at[index])
        for index, (source, target) in enumerate(
            ((labels, label_in), (weights, weight_in), (owner_of, owner_in))
        )
    ]
    for copy in inputs:
        copy.start()
    incoming = []
    for pair in range(pairs):
        for which, source in enumerate((vis_real, vis_imag)):
            copy = pltpu.make_async_copy(
                source.at[:, pl.ds(2 * pair, 2)], fresh.at[pair, which], loads.at[pair, which]
            )
            copy.start()
            incoming.append(copy)

    barrier = pltpu.get_barrier_semaphore()
    for hop in range(1, N):
        pl.semaphore_signal(
            barrier, inc=1, device_id={"bl": lax.rem(me + hop, N)}, device_id_type=MESH
        )
    for hop in range(1, p.parts):
        pl.semaphore_signal(
            barrier, inc=1, device_id={"tm": lax.rem(here + hop, p.parts)}, device_id_type=MESH
        )

    spread = (iota((R, both), 1) // 2 == iota((R, both), 0)).astype(F32).astype(BF16)
    before = (iota((G, G), 0) < iota((G, G), 1)).astype(F32).astype(BF16)
    for copy in inputs:
        copy.wait()
    label = jnp.concatenate(
        [label_in[i : i + 1] for i in range(label_in.shape[0])], axis=1
    )
    base = jnp.concatenate(
        [
            (label // 256).astype(F32),
            lax.rem(label, 256).astype(F32),
            weight_in[...].astype(F32),
            jnp.zeros((-(T + 2) % 8, R), F32),
        ],
        axis=0,
    )
    doubled = dot(base.astype(BF16), spread)
    label_twice = (doubled[0:1] * 256.0 + doubled[1:2]).astype(I32)
    hit = (iota((G, both), 0) == label_twice).astype(F32).astype(BF16)
    count = lax.dot_general(
        jnp.ones((8, both), BF16), hit, (((1,), (1,)), ((), ())), preferred_element_type=F32
    )
    present = (count[0:1] > 0.5).astype(F32)
    owner = owner_in[...]
    owned = (iota((N, G), 0) == owner).astype(F32)
    earlier = dot(jnp.concatenate([owned, owned * present], axis=0).astype(BF16), before)
    rank = jnp.sum(owned * earlier[:N], axis=0, keepdims=True)
    order = jnp.sum(owned * earlier[N:], axis=0, keepdims=True)
    info = jnp.concatenate([owner.astype(F32), order, jnp.zeros((6, G), F32)], axis=0)
    placed = dot(info.astype(BF16), hit)
    row_owner = placed[0:1].astype(I32)
    row_order = placed[1:2].astype(I32)
    second = lax.rem(iota((1, both), 1), 2)

    listed = order.astype(I32)
    seen = present > 0.5
    rank_main = rank_tail = None
    if p.main:
        slot_main = jnp.where(seen & (listed < p.main), owner * p.main + listed, -1)
        rank_main = jnp.sum(
            jnp.where(iota((p.mains, G), 0) == slot_main, rank, 0.0), axis=1, keepdims=True
        )
    if p.extra:
        slot_tail = jnp.where(
            seen & (listed >= p.main), owner * p.extra + listed - p.main, -1
        )
        row = iota((p.tails, 1), 0)
        within = lax.rem(row, p.tail)
        slot_of_row = row // p.tail * p.extra + lax.rem(within, p.extra)
        rank_tail = jnp.sum(
            jnp.where((slot_of_row == slot_tail) & (within < p.extra * T), rank, 0.0),
            axis=1,
            keepdims=True,
        )

    def laid(column, height, offset):
        shape = (column.shape[0], 128)
        match = lax.rem(iota(shape, 0), height) == iota(shape, 1) - offset
        block = jnp.where(match, jnp.broadcast_to(column, shape), 0.0)
        return jnp.sum(block.reshape(shape[0] // height, height, 128), axis=1, keepdims=True)

    base_tail = T * p.main
    note = jnp.zeros((N, 1, 128), F32)

    def start(kind, peer):
        if kind < T:
            pieces = [(send.at[kind], came.at[kind], kind)]
            pieces.append((send_step.at[kind], came_step.at[kind], T + kind))
        else:
            pieces = [(send_note, came_note, 2 * T + 1)]
            if p.extra:
                pieces.append((send_tail, came_tail, 2 * T))
        return [
            pltpu.make_async_remote_copy(
                src_ref=source.at[peer],
                dst_ref=target.at[me],
                send_sem=sends.at[index, peer],
                recv_sem=arrivals.at[index, me],
                device_id={"bl": peer},
                device_id_type=MESH,
            )
            for source, target, index in pieces
        ]

    def arrive(kind, source):
        if kind < T:
            pieces = [(send.at[kind], came.at[kind], kind)]
            pieces.append((send_step.at[kind], came_step.at[kind], T + kind))
        else:
            pieces = [(send_note, came_note, 2 * T + 1)]
            if p.extra:
                pieces.append((send_tail, came_tail, 2 * T))
        return [
            pltpu.make_async_remote_copy(
                src_ref=origin.at[source],
                dst_ref=target.at[source],
                send_sem=sends.at[index, source],
                recv_sem=arrivals.at[index, source],
                device_id={"bl": source},
                device_id_type=MESH,
            )
            for origin, target, index in pieces
        ]

    def post(kind, peer):
        for copy in start(kind, peer):
            copy.start()

    def encode(real, imag):
        peak = jnp.maximum(
            jnp.max(jnp.abs(real), axis=1, keepdims=True),
            jnp.max(jnp.abs(imag), axis=1, keepdims=True),
        )
        step = jnp.maximum(peak, 1e-30) * (1.0078125 / 32767.0)
        step = step.astype(BF16).astype(F32)
        invert = 1.0 / step
        code_real = jnp.round(real * invert).astype(I32)
        code_imag = jnp.round(imag * invert).astype(I32)
        return (code_real << 16) | (code_imag & 65535), step

    def encode_main(time, o):
        at = pl.multiple_of(time % 2 * p.mains + o * p.main, 16)
        rows = pl.ds(at, p.main)
        code, step = encode(part[time // 2, 0, rows], part[time // 2, 1, rows])
        return code, laid(step, p.main, 0)[0]

    def handle_main(time):
        def one(step, carry):
            peer = partner(me, step, N)
            code, steps = encode_main(time, peer)
            send[time, peer] = code
            send_step[time, peer] = steps
            post(time, peer)
            return carry

        lax.fori_loop(1, N, one, 0)
        code, steps = encode_main(time, me)
        came[time, me] = code
        came_step[time, me] = steps

    def encode_tail(o):
        at = pl.multiple_of(o * p.tail, 8)
        code, step = encode(part_tail[0, pl.ds(at, p.tail)], part_tail[1, pl.ds(at, p.tail)])
        return code, send_note[o] + laid(step, p.tail, base_tail + p.tail)[0]

    def handle_tail():
        def one(step, carry):
            peer = partner(me, step, N)
            if p.extra:
                code, facts = encode_tail(peer)
                send_tail[peer] = code
                send_note[peer] = facts
            post(T, peer)
            return carry

        lax.fori_loop(1, N, one, 0)
        if p.extra:
            code, facts = encode_tail(me)
            came_tail[me] = code
            came_note[me] = facts
        else:
            came_note[me] = send_note[me]

    all_rows = 2 * p.mains + p.tails
    tail_weight = jnp.zeros((p.tails, 1), F32)
    for pair in range(pairs):
        weight = jnp.where(
            second == 0, doubled[2 + 2 * pair : 3 + 2 * pair], doubled[3 + 2 * pair : 4 + 2 * pair]
        )
        target = jnp.where(
            row_order < p.main,
            second * p.mains + row_owner * p.main + row_order,
            2 * p.mains
            + row_owner * p.tail
            + (2 * pair + second) * p.extra
            + row_order
            - p.main,
        )
        folder = jnp.where(iota((all_rows, both), 0) == target, weight, 0.0)
        sums = jnp.sum(folder, axis=1, keepdims=True)
        folder = folder.astype(BF16)
        for copy in incoming[2 * pair : 2 * pair + 2]:
            copy.wait()
        for which in range(2):
            made = dot(folder, fresh[pair, which].reshape(both, F))
            if p.main:
                part[pair, which] = made[: 2 * p.mains]
            if p.extra:
                if pair:
                    part_tail[which] += made[2 * p.mains :]
                else:
                    part_tail[which] = made[2 * p.mains :]
        if p.main:
            for which in range(2):
                fact = sums[which * p.mains : (which + 1) * p.mains] * n + rank_main
                note = note + laid(fact, p.main, (2 * pair + which) * p.main)
        if p.extra:
            tail_weight = tail_weight + sums[2 * p.mains :]
        if pair == 0:
            pl.semaphore_wait(barrier, N + p.parts - 2)
            if p.main:
                handle_main(0)
        if pair == pairs - 1:
            if p.extra:
                note = note + laid(tail_weight * n + rank_tail, p.tail, base_tail)
            send_note[...] = note
            handle_tail()
            if p.main:
                handle_main(1)
        if p.main and pair:
            handle_main(2 * pair)
            handle_main(2 * pair + 1)

    turn = 2.0 * math.pi / F
    phase = turn * iota((1, F), 1).astype(F32)
    shape = (
        HARRIS[0]
        - HARRIS[1] * jnp.cos(phase)
        + HARRIS[2] * jnp.cos(2.0 * phase)
        - HARRIS[3] * jnp.cos(3.0 * phase)
    )
    taper[...] = shape / jnp.sqrt(jnp.sum(shape * shape, axis=1, keepdims=True))
    fine = 16
    for q in range(RADIX):
        delay = RADIX * iota((fine, short), 1) + q
        low = turn * lax.rem(iota((fine, short), 0) * delay, F).astype(F32)
        high = turn * lax.rem(fine * iota((fine, short), 0) * delay, F).astype(F32)
        low_cos, low_sin = jnp.cos(low), jnp.sin(low)
        high_cos, high_sin = jnp.cos(high), jnp.sin(high)
        for a in range(short // fine):
            ac, as_ = high_cos[a : a + 1], high_sin[a : a + 1]
            rows = pl.ds(a * fine, fine)
            upper, lower = halves(ac * low_cos - as_ * low_sin)
            table[q, 0, rows, :short] = upper
            table[q, 1, rows, :short] = lower
            upper, lower = halves(as_ * low_cos + ac * low_sin)
            table[q, 0, rows, short:] = upper
            table[q, 1, rows, short:] = lower

    def wait_for(kind, source):
        for copy in arrive(kind, source):
            copy.wait_recv()

    def split(code):
        imag = (code << 16) >> 16
        parts = (code >> 24, (code >> 16) & 255, imag >> 8, imag & 255)
        return [part.astype(F32).astype(BF16) for part in parts]

    def gathered(values, height, offset):
        values = values.reshape(N, 128)
        blocks = []
        for block in range(lanes(N * height) // 128):
            lane = iota((N, 128), 1) + block * 128
            picked = jnp.take_along_axis(values, offset + lax.rem(lane, height), axis=1)
            mine = lane // height == iota((N, 128), 0)
            blocks.append(jnp.sum(jnp.where(mine, picked, 0.0), axis=0, keepdims=True))
        return jnp.concatenate(blocks, axis=1)[:, : N * height]

    def facts_of(values, height, offset):
        fact = gathered(values, height, offset).astype(I32)
        return lax.rem(fact, n), (fact // n).astype(F32)

    for step in range(1, N):
        wait_for(T, partner(me, step, N))
    notes = came_note[...]
    rank_row = iota((n, 1), 0)
    main_facts = []
    if p.main:
        main_facts = [facts_of(notes, p.main, time * p.main) for time in range(T)]
    tail_sums = []
    if p.extra:
        tail_rank, tail_heft = facts_of(notes, p.tail, base_tail)
        tail_step = gathered(notes, p.tail, base_tail + p.tail)
        pieces = split(came_tail[...].reshape(p.tails, F))
        lane = lax.rem(iota((1, p.tails), 1), p.tail)
        lane_time = jnp.where(lane < p.extra * T, lane // p.extra, T)
        selectors = []
        for time in range(T):
            chosen = (rank_row == tail_rank) & (lane_time == time)
            selector = jnp.where(chosen, tail_step, 0.0)
            selectors.append(jnp.concatenate([256.0 * selector, selector], axis=1))
            tail_sums.append(jnp.sum(jnp.where(chosen, tail_heft, 0.0), axis=1, keepdims=True))
        selectors = jnp.concatenate(selectors, axis=0).astype(BF16)
        total[0] = dot(selectors, jnp.concatenate(pieces[:2], axis=0))
        total[1] = dot(selectors, jnp.concatenate(pieces[2:], axis=0))

    ahead = pltpu.make_async_remote_copy(
        src_ref=spectrum.at[0],
        dst_ref=following,
        send_sem=ahead_sems.at[0],
        recv_sem=ahead_sems.at[1],
        device_id={"tm": lax.rem(here + p.parts - 1, p.parts)},
        device_id_type=MESH,
    )
    rows = n // p.parts

    def across(hop, q):
        return pltpu.make_async_remote_copy(
            src_ref=share.at[lax.rem(here + hop, p.parts), q],
            dst_ref=shared.at[hop - 1, q],
            send_sem=tail_sends.at[hop - 1, q],
            recv_sem=tail_arrivals.at[hop - 1, q],
            device_id={"tm": lax.rem(here + hop, p.parts)},
            device_id_type=MESH,
        )

    def power_of(product):
        return (product[:, :short] + product[:, short:]).reshape(p.parts, rows, short)

    for time in range(T):
        weight_sum = jnp.zeros((n, 1), F32)
        if p.extra:
            weight_sum = weight_sum + tail_sums[time]
        if p.main:

            def unpack(source):
                for which, piece in enumerate(split(came[time, source])):
                    at = which % 2 * p.mains + source * p.main
                    planes[which // 2, pl.ds(pl.multiple_of(at, 16), p.main)] = piece

            def one(step, carry):
                source = partner(me, step, N)
                wait_for(time, source)
                unpack(source)
                return carry

            unpack(me)
            lax.fori_loop(1, N, one, 0)
            rank, heft = main_facts[time]
            chosen = rank_row == rank
            selector = jnp.where(chosen, gathered(came_step[time], p.main, 0), 0.0)
            selector = jnp.concatenate([256.0 * selector, selector], axis=1).astype(BF16)
            weight_sum = weight_sum + jnp.sum(jnp.where(chosen, heft, 0.0), axis=1, keepdims=True)
            real, imag = dot(selector, planes[0]), dot(selector, planes[1])
        block = pl.ds(time * n, n)
        if p.main and p.extra:
            real, imag = real + total[0, block], imag + total[1, block]
        elif p.extra:
            real, imag = total[0, block], total[1, block]
        scale = 1.0 / jnp.maximum(weight_sum, 1.0)
        window = taper[...]
        real = real * scale * window
        imag = imag * scale * window
        r = [real[:, i * short : (i + 1) * short] for i in range(RADIX)]
        m = [imag[:, i * short : (i + 1) * short] for i in range(RADIX)]
        er, ei, fr, fi = r[0] + r[2], m[0] + m[2], r[1] + r[3], m[1] + m[3]
        gr, gi, hr, hi = r[0] - r[2], m[0] - m[2], r[1] - r[3], m[1] - m[3]
        folded = (
            (er + fr, ei + fi),
            (gr + hi, gi - hr),
            (er - fr, ei - fi),
            (gr - hi, gi + hr),
        )
        if time == T - 1:
            ahead.wait()
        for q in range(RADIX):
            upper, lower = halves(jnp.concatenate(folded[q], axis=0))
            first = dot(jnp.concatenate([upper, lower], axis=0), table[q, 0])
            wave = first[: 2 * n] + first[2 * n :] + dot(upper, table[q, 1])
            now = jnp.concatenate(
                [wave[:n, :short] + wave[n:, short:], wave[n:, :short] - wave[:n, short:]],
                axis=1,
            )
            spectrum[time, q] = now
            if time:
                power = power_of(spectrum[time - 1, q] * now)
                if time > 1:
                    power = power + share[:, q]
                if time == T - 1:
                    beyond = power_of(now * following[q])
                    power = power + jnp.where(here < p.parts - 1, beyond, 0.0)
                share[:, q] = power
                if time == T - 1:
                    for hop in range(1, p.parts):
                        across(hop, q).start()
        if time == 0:
            ahead.start()

    for kind in range(T + 1):
        if kind == T or p.main:
            for step in range(1, N):
                for copy in start(kind, partner(me, step, N)):
                    copy.wait_send()
    summed = []
    for q in range(RADIX):
        value = share[here, q]
        for hop in range(1, p.parts):
            across(hop, q).wait()
            value = value + shared[hop - 1, q]
        summed.append(value)
    lane = iota((rows, 128), 1)
    for tile in range(F // 128):
        begin = tile * 128 // RADIX
        block = begin // 128 * 128
        index = lane // RADIX + (begin - block)
        value = None
        for q in range(RADIX):
            picked = jnp.take_along_axis(summed[q][:, block : block + 128], index, axis=1)
            value = picked if value is None else jnp.where(lax.rem(lane, RADIX) == q, picked, value)
        out[:, tile * 128 : (tile + 1) * 128] = value


def per_device(visibility_real, visibility_imag, weights, labels, owner_of):
    row_count, times, channels = visibility_real.shape
    owners, parts = lax.axis_size("bl"), lax.axis_size("tm")
    p = Plan(row_count, times, channels, owner_of.shape[0], owners, parts)
    short = channels // RADIX
    inside = pl.BlockSpec(memory_space=pltpu.VMEM)
    outside = pl.BlockSpec(memory_space=pltpu.HBM)
    some = lambda count: max(count, 8)
    main, tail = some(p.main), some(p.tail)
    rows = p.per_owner // parts
    return pl.pallas_call(
        functools.partial(program_kernel, p),
        out_shape=jax.ShapeDtypeStruct((rows, channels), F32),
        in_specs=[outside] * 5,
        out_specs=inside,
        scratch_shapes=[
            pltpu.VMEM((times, row_count), I32),
            pltpu.VMEM((row_count // 128, 128), I32),
            pltpu.VMEM((1, p.groups), I32),
            pltpu.VMEM((times // 2, 2, row_count, 2, channels), BF16),
            pltpu.VMEM((times // 2, 2, some(2 * p.mains), channels), F32),
            pltpu.VMEM((2, some(p.tails), channels), F32),
            pltpu.VMEM((times, owners, main, channels), I32),
            pltpu.VMEM((owners, tail, channels), I32),
            pltpu.VMEM((owners, 1, 128), F32),
            pltpu.VMEM((times, owners, 1, 128), F32),
            pltpu.VMEM((times, owners, main, channels), I32),
            pltpu.VMEM((owners, tail, channels), I32),
            pltpu.VMEM((owners, 1, 128), F32),
            pltpu.VMEM((times, owners, 1, 128), F32),
            pltpu.VMEM((RADIX, 2, short, 2 * short), BF16),
            pltpu.VMEM((1, channels), F32),
            pltpu.VMEM((2, times * p.per_owner, channels), F32),
            pltpu.VMEM((2, some(2 * p.mains), channels), BF16),
            pltpu.VMEM((times, RADIX, p.per_owner, 2 * short), F32),
            pltpu.VMEM((RADIX, p.per_owner, 2 * short), F32),
            pltpu.VMEM((parts, RADIX, rows, short), F32),
            pltpu.VMEM((parts - 1, RADIX, rows, short), F32),
            pltpu.SemaphoreType.DMA((times // 2, 2)),
            pltpu.SemaphoreType.DMA((3,)),
            pltpu.SemaphoreType.DMA((2 * times + 2, owners)),
            pltpu.SemaphoreType.DMA((2 * times + 2, owners)),
            pltpu.SemaphoreType.DMA((2,)),
            pltpu.SemaphoreType.DMA((parts - 1, RADIX)),
            pltpu.SemaphoreType.DMA((parts - 1, RADIX)),
        ],
        compiler_params=pltpu.CompilerParams(
            collective_id=0, has_side_effects=True, vmem_limit_bytes=60 * 2**20
        ),
    )(visibility_real, visibility_imag, weights.T, labels.reshape(-1, 128), owner_of[None, :])


def solution(mesh):
    placed = (P("bl", "tm", None), P("bl", "tm", None), P("bl", "tm"), P("bl"), P())
    return jax.shard_map(
        per_device, mesh=mesh, in_specs=placed, out_specs=P(("bl", "tm"), None), check_vma=False
    )
```

```python
import functools
import math

import jax
import jax.numpy as jnp
from jax import lax
from jax.experimental import pallas as pl
from jax.experimental.pallas import tpu as pltpu
from jax.sharding import PartitionSpec as P

HARRIS = (0.35875, 0.48829, 0.14128, 0.01168)
RADIX = 4
F32, BF16, I32 = jnp.float32, jnp.bfloat16, jnp.int32
MESH = pl.DeviceIdType.MESH


def iota(shape, dim):
    return lax.broadcasted_iota(I32, shape, dim)


def dot(a, b):
    return jnp.dot(a, b, preferred_element_type=F32)


def halves(value):
    high = value.astype(BF16)
    return high, (value - high.astype(F32)).astype(BF16)


def lanes(count):
    return -(-max(count, 1) // 128) * 128


def partner(me, step, size):
    if size & (size - 1):
        return lax.rem(me + step, size)
    peer, bit = 0, 1
    while bit < size:
        peer = peer + bit * lax.rem(lax.rem(me // bit, 2) + step // bit, 2)
        bit *= 2
    return peer


class Plan:
    def __init__(self, row_count, times, channels, groups, owners, parts):
        capacity = 3 * row_count // (2 * owners)
        self.rows, self.times, self.channels, self.groups = row_count, times, channels, groups
        self.owners, self.parts = owners, parts
        self.per_owner = groups // owners
        self.distinct = min(capacity // 4, self.per_owner // 2)
        self.main = self.distinct // 16 * 16
        self.extra = self.distinct - self.main
        self.tail = -(-self.extra * times // 8) * 8
        self.mains = owners * self.main
        self.tails = owners * self.tail
        assert times * self.main + self.tail <= 128


def program_kernel(
    plan, vis_real, vis_imag, weights, labels, owner_of, out,
    weight_in, label_in, owner_in,
    fresh, part, part_tail, send, send_tail, send_note,
    came, came_tail, came_note,
    table, taper, total, planes, spectrum, following, share, shared,
    loads, small, sends, arrivals, ahead_sems, tail_sends, tail_arrivals,
):
    p = plan
    T, N, F, G, R = p.times, p.owners, p.channels, p.groups, p.rows
    pairs, both = T // 2, 2 * R
    short = F // RADIX
    n = p.per_owner
    me = lax.axis_index("bl")
    here = lax.axis_index("tm")

    inputs = [
        pltpu.make_async_copy(source, target, small.at[index])
        for index, (source, target) in enumerate(
            ((labels, label_in), (weights, weight_in), (owner_of, owner_in))
        )
    ]
    for copy in inputs:
        copy.start()
    incoming = []
    for pair in range(pairs):
        for which, source in enumerate((vis_real, vis_imag)):
            copy = pltpu.make_async_copy(
                source.at[:, pl.ds(2 * pair, 2)], fresh.at[pair, which], loads.at[pair, which]
            )
            incoming.append(copy)
    for copy in incoming[:2]:
        copy.start()

    barrier = pltpu.get_barrier_semaphore()
    for hop in range(1, N):
        pl.semaphore_signal(
            barrier, inc=1, device_id={"bl": lax.rem(me + hop, N)}, device_id_type=MESH
        )
    for hop in range(1, p.parts):
        pl.semaphore_signal(
            barrier, inc=1, device_id={"tm": lax.rem(here + hop, p.parts)}, device_id_type=MESH
        )

    spread = (iota((R, both), 1) // 2 == iota((R, both), 0)).astype(F32).astype(BF16)
    before = (iota((G, G), 0) < iota((G, G), 1)).astype(F32).astype(BF16)
    for copy in inputs:
        copy.wait()
    label = jnp.concatenate(
        [label_in[i : i + 1] for i in range(label_in.shape[0])], axis=1
    )
    base = jnp.concatenate(
        [
            (label // 256).astype(F32),
            lax.rem(label, 256).astype(F32),
            weight_in[...].astype(F32),
            jnp.zeros((-(T + 2) % 8, R), F32),
        ],
        axis=0,
    )
    doubled = dot(base.astype(BF16), spread)
    label_twice = (doubled[0:1] * 256.0 + doubled[1:2]).astype(I32)
    hit = (iota((G, both), 0) == label_twice).astype(F32).astype(BF16)
    count = lax.dot_general(
        jnp.ones((8, both), BF16), hit, (((1,), (1,)), ((), ())), preferred_element_type=F32
    )
    present = (count[0:1] > 0.5).astype(F32)
    owner = owner_in[...]
    owned = (iota((N, G), 0) == owner).astype(F32)
    earlier = dot(jnp.concatenate([owned, owned * present], axis=0).astype(BF16), before)
    rank = jnp.sum(owned * earlier[:N], axis=0, keepdims=True)
    order = jnp.sum(owned * earlier[N:], axis=0, keepdims=True)
    info = jnp.concatenate([owner.astype(F32), order, jnp.zeros((6, G), F32)], axis=0)
    placed = dot(info.astype(BF16), hit)
    row_owner = placed[0:1].astype(I32)
    row_order = placed[1:2].astype(I32)
    second = lax.rem(iota((1, both), 1), 2)

    listed = order.astype(I32)
    seen = present > 0.5
    rank_main = rank_tail = None
    if p.main:
        slot_main = jnp.where(seen & (listed < p.main), owner * p.main + listed, -1)
        rank_main = jnp.sum(
            jnp.where(iota((p.mains, G), 0) == slot_main, rank, 0.0), axis=1, keepdims=True
        )
    if p.extra:
        slot_tail = jnp.where(
            seen & (listed >= p.main), owner * p.extra + listed - p.main, -1
        )
        row = iota((p.tails, 1), 0)
        within = lax.rem(row, p.tail)
        slot_of_row = row // p.tail * p.extra + lax.rem(within, p.extra)
        rank_tail = jnp.sum(
            jnp.where((slot_of_row == slot_tail) & (within < p.extra * T), rank, 0.0),
            axis=1,
            keepdims=True,
        )

    def laid(column, height, offset):
        shape = (column.shape[0], 128)
        match = lax.rem(iota(shape, 0), height) == iota(shape, 1) - offset
        block = jnp.where(match, jnp.broadcast_to(column, shape), 0.0)
        return jnp.sum(block.reshape(shape[0] // height, height, 128), axis=1, keepdims=True)

    base_tail = T * p.main
    note = jnp.zeros((N, 1, 128), F32)
    send_note[...] = jnp.zeros_like(send_note)

    def start(kind, peer):
        if kind < T:
            pieces = [(send.at[kind], came.at[kind], kind)]
        else:
            pieces = [(send_note, came_note, T + 1)]
            if p.extra:
                pieces.append((send_tail, came_tail, T))
        return [
            pltpu.make_async_remote_copy(
                src_ref=source.at[peer],
                dst_ref=target.at[me],
                send_sem=sends.at[index, peer],
                recv_sem=arrivals.at[index, me],
                device_id={"bl": peer},
                device_id_type=MESH,
            )
            for source, target, index in pieces
        ]

    def arrive(kind, source):
        if kind < T:
            pieces = [(send.at[kind], came.at[kind], kind)]
        else:
            pieces = [(send_note, came_note, T + 1)]
            if p.extra:
                pieces.append((send_tail, came_tail, T))
        return [
            pltpu.make_async_remote_copy(
                src_ref=origin.at[source],
                dst_ref=target.at[source],
                send_sem=sends.at[index, source],
                recv_sem=arrivals.at[index, source],
                device_id={"bl": source},
                device_id_type=MESH,
            )
            for origin, target, index in pieces
        ]

    def post(kind, peer):
        for copy in start(kind, peer):
            copy.start()

    def encode(real, imag):
        peak = jnp.maximum(
            jnp.max(jnp.abs(real), axis=1, keepdims=True),
            jnp.max(jnp.abs(imag), axis=1, keepdims=True),
        )
        step = jnp.maximum(peak, 1e-30) * (1.0078125 / 32767.0)
        step = step.astype(BF16).astype(F32)
        invert = 1.0 / step
        code_real = jnp.round(real * invert).astype(I32)
        code_imag = jnp.round(imag * invert).astype(I32)
        return (code_real << 16) | (code_imag & 65535), step

    def encode_main(time, o):
        at = pl.multiple_of(time % 2 * p.mains + o * p.main, 16)
        rows = pl.ds(at, p.main)
        code, step = encode(part[time // 2, 0, rows], part[time // 2, 1, rows])
        send_note[o, 1:2] += laid(step, p.main, time * p.main)[0]
        return code

    def encode_tail(o):
        rows = pl.ds(pl.multiple_of(o * p.tail, 8), p.tail)
        code, step = encode(part_tail[0, rows], part_tail[1, rows])
        send_note[o, 1:2] += laid(step, p.tail, base_tail)[0]
        return code

    def handle_main(time, now):
        def one(step, carry):
            peer = partner(me, step, N)
            send[time, peer] = encode_main(time, peer)
            if now:
                post(time, peer)
            return carry

        if now:
            lax.fori_loop(N // 2, N, one, 0)
            lax.fori_loop(1, N // 2, one, 0)
        else:
            lax.fori_loop(1, N, one, 0)
        came[time, me] = encode_main(time, me)

    def handle_tail():
        def one(step, carry):
            peer = partner(me, step, N)
            send_tail[peer] = encode_tail(peer)
            return carry

        lax.fori_loop(1, N, one, 0)
        came_tail[me] = encode_tail(me)

    all_rows = 2 * p.mains + p.tails
    tail_weight = jnp.zeros((p.tails, 1), F32)
    for pair in range(pairs):
        weight = jnp.where(
            second == 0, doubled[2 + 2 * pair : 3 + 2 * pair], doubled[3 + 2 * pair : 4 + 2 * pair]
        )
        target = jnp.where(
            row_order < p.main,
            second * p.mains + row_owner * p.main + row_order,
            2 * p.mains
            + row_owner * p.tail
            + (2 * pair + second) * p.extra
            + row_order
            - p.main,
        )
        folder = jnp.where(iota((all_rows, both), 0) == target, weight, 0.0)
        sums = jnp.sum(folder, axis=1, keepdims=True)
        folder = folder.astype(BF16)
        for copy in incoming[2 * pair : 2 * pair + 2]:
            copy.wait()
        for copy in incoming[2 * pair + 2 : 2 * pair + 4]:
            copy.start()
        bounds = [0, all_rows]
        if pair == 0 and p.main:
            bounds = [0, p.mains, all_rows]
        for low, high in zip(bounds, bounds[1:]):
            for which in range(2):
                made = dot(folder[low:high], fresh[pair, which].reshape(both, F))
                middle = max(2 * p.mains - low, 0)
                if middle:
                    part[pair, which, low : min(high, 2 * p.mains)] = made[:middle]
                if p.extra and high == all_rows:
                    if pair:
                        part_tail[which] += made[middle:]
                    else:
                        part_tail[which] = made[middle:]
            if pair == 0 and low == 0:
                pl.semaphore_wait(barrier, N + p.parts - 2)
                if p.main:
                    handle_main(0, True)
        if p.main:
            for which in range(2):
                fact = sums[which * p.mains : (which + 1) * p.mains] * n + rank_main
                note = note + laid(fact, p.main, (2 * pair + which) * p.main)
        if p.extra:
            tail_weight = tail_weight + sums[2 * p.mains :]
        if p.main:
            for time in range(max(2 * pair, 1), 2 * pair + 2):
                handle_main(time, False)
    if p.extra:
        note = note + laid(tail_weight * n + rank_tail, p.tail, base_tail)
        handle_tail()
    send_note[:, 0:1] = note
    came_note[me] = send_note[me]
    for kind in [T] + list(range(1, T if p.main else 1)):
        for step in range(1, N):
            post(kind, partner(me, step, N))

    turn = 2.0 * math.pi / F
    phase = turn * iota((1, F), 1).astype(F32)
    shape = (
        HARRIS[0]
        - HARRIS[1] * jnp.cos(phase)
        + HARRIS[2] * jnp.cos(2.0 * phase)
        - HARRIS[3] * jnp.cos(3.0 * phase)
    )
    taper[...] = shape / jnp.sqrt(jnp.sum(shape * shape, axis=1, keepdims=True))
    fine = 16
    for q in range(RADIX):
        delay = RADIX * iota((fine, short), 1) + q
        low = turn * lax.rem(iota((fine, short), 0) * delay, F).astype(F32)
        high = turn * lax.rem(fine * iota((fine, short), 0) * delay, F).astype(F32)
        low_cos, low_sin = jnp.cos(low), jnp.sin(low)
        high_cos, high_sin = jnp.cos(high), jnp.sin(high)
        for a in range(short // fine):
            ac, as_ = high_cos[a : a + 1], high_sin[a : a + 1]
            rows = pl.ds(a * fine, fine)
            upper, lower = halves(ac * low_cos - as_ * low_sin)
            table[q, 0, rows, :short] = upper
            table[q, 1, rows, :short] = lower
            upper, lower = halves(as_ * low_cos + ac * low_sin)
            table[q, 0, rows, short:] = upper
            table[q, 1, rows, short:] = lower

    def wait_for(kind, source):
        for copy in arrive(kind, source):
            copy.wait_recv()

    cut = 1 if N & (N - 1) else 2
    group = N // cut
    mine = me // group

    def split(code):
        imag = (code << 16) >> 16
        parts = (code >> 24, (code >> 16) & 255, imag >> 8, imag & 255)
        return [part.astype(F32).astype(BF16) for part in parts]

    def gathered(values, height, offset):
        values = values.reshape(N, 128)
        blocks = []
        for block in range(lanes(N * height) // 128):
            lane = iota((N, 128), 1) + block * 128
            picked = jnp.take_along_axis(values, offset + lax.rem(lane, height), axis=1)
            mine = lane // height == iota((N, 128), 0)
            blocks.append(jnp.sum(jnp.where(mine, picked, 0.0), axis=0, keepdims=True))
        return jnp.concatenate(blocks, axis=1)[:, : N * height]

    def facts_of(values, height, offset):
        fact = gathered(values, height, offset).astype(I32)
        return lax.rem(fact, n), (fact // n).astype(F32)

    for step in range(1, N):
        wait_for(T, partner(me, step, N))
    facts, steps = came_note[:, 0], came_note[:, 1]
    rank_row = iota((n, 1), 0)
    main_picks = []
    if p.main:
        for time in range(T):
            rank, heft = facts_of(facts, p.main, time * p.main)
            chosen = rank_row == rank
            heft = jnp.sum(jnp.where(chosen, heft, 0.0), axis=1, keepdims=True)
            selector = jnp.where(chosen, gathered(steps, p.main, time * p.main), 0.0)
            main_picks.append((selector, heft))
    tail_sums = []
    if p.extra:
        tail_rank, tail_heft = facts_of(facts, p.tail, base_tail)
        tail_step = gathered(steps, p.tail, base_tail)
        pieces = split(came_tail[...].reshape(p.tails, F))
        lane = lax.rem(iota((1, p.tails), 1), p.tail)
        lane_time = jnp.where(lane < p.extra * T, lane // p.extra, T)
        selectors = []
        for time in range(T):
            chosen = (rank_row == tail_rank) & (lane_time == time)
            selector = jnp.where(chosen, tail_step, 0.0)
            selectors.append(jnp.concatenate([256.0 * selector, selector], axis=1))
            tail_sums.append(jnp.sum(jnp.where(chosen, tail_heft, 0.0), axis=1, keepdims=True))
        selectors = jnp.concatenate(selectors, axis=0).astype(BF16)
        total[0] = dot(selectors, jnp.concatenate(pieces[:2], axis=0))
        total[1] = dot(selectors, jnp.concatenate(pieces[2:], axis=0))

    ahead = pltpu.make_async_remote_copy(
        src_ref=spectrum.at[0],
        dst_ref=following,
        send_sem=ahead_sems.at[0],
        recv_sem=ahead_sems.at[1],
        device_id={"tm": lax.rem(here + p.parts - 1, p.parts)},
        device_id_type=MESH,
    )
    rows = n // p.parts

    def across(hop, q):
        return pltpu.make_async_remote_copy(
            src_ref=share.at[lax.rem(here + hop, p.parts), q],
            dst_ref=shared.at[hop - 1, q],
            send_sem=tail_sends.at[hop - 1, q],
            recv_sem=tail_arrivals.at[hop - 1, q],
            device_id={"tm": lax.rem(here + hop, p.parts)},
            device_id_type=MESH,
        )

    def power_of(product):
        return (product[:, :short] + product[:, short:]).reshape(p.parts, rows, short)

    for time in range(T):
        weight_sum = jnp.zeros((n, 1), F32)
        if p.extra:
            weight_sum = weight_sum + tail_sums[time]
        if p.main:

            selector_all, heft = main_picks[time]
            weight_sum = weight_sum + heft
            real = imag = 0.0
            if p.extra:
                block = pl.ds(time * n, n)
                real, imag = total[0, block], total[1, block]
            wide = group * p.main
            for near in range(cut):
                members = range(near * group, (near + 1) * group)
                for step in members:
                    source = partner(me, step, N) if step else me
                    if step:
                        wait_for(time, source)
                    for which, piece in enumerate(split(came[time, source])):
                        at = which % 2 * wide + lax.rem(source, group) * p.main
                        at = pl.ds(pl.multiple_of(at, 16), p.main)
                        planes[near, which // 2, at] = piece
                selector = selector_all
                if cut == 2:
                    selector = jnp.where(
                        (mine + near) % 2 == 0, selector[:, :wide], selector[:, wide:]
                    )
                selector = jnp.concatenate([256.0 * selector, selector], axis=1).astype(BF16)
                real = real + dot(selector, planes[near, 0])
                imag = imag + dot(selector, planes[near, 1])
        else:
            block = pl.ds(time * n, n)
            real, imag = total[0, block], total[1, block]
        scale = 1.0 / jnp.maximum(weight_sum, 1.0)
        window = taper[...]
        real = real * scale * window
        imag = imag * scale * window
        r = [real[:, i * short : (i + 1) * short] for i in range(RADIX)]
        m = [imag[:, i * short : (i + 1) * short] for i in range(RADIX)]
        er, ei, fr, fi = r[0] + r[2], m[0] + m[2], r[1] + r[3], m[1] + m[3]
        gr, gi, hr, hi = r[0] - r[2], m[0] - m[2], r[1] - r[3], m[1] - m[3]
        folded = (
            (er + fr, ei + fi),
            (gr + hi, gi - hr),
            (er - fr, ei - fi),
            (gr - hi, gi + hr),
        )
        if time == T - 1:
            ahead.wait()
        for q in range(RADIX):
            upper, lower = halves(jnp.concatenate(folded[q], axis=0))
            first = dot(jnp.concatenate([upper, lower], axis=0), table[q, 0])
            wave = first[: 2 * n] + first[2 * n :] + dot(upper, table[q, 1])
            now = jnp.concatenate(
                [wave[:n, :short] + wave[n:, short:], wave[n:, :short] - wave[:n, short:]],
                axis=1,
            )
            spectrum[time, q] = now
            if time:
                power = power_of(spectrum[time - 1, q] * now)
                if time > 1:
                    power = power + share[:, q]
                if time == T - 1:
                    beyond = power_of(now * following[q])
                    power = power + jnp.where(here < p.parts - 1, beyond, 0.0)
                share[:, q] = power
                if time == T - 1 and q % 2 == 1:
                    for part_q in range(q - 1, q + 1):
                        for hop in range(1, p.parts):
                            across(hop, part_q).start()
        if time == 0:
            ahead.start()

    for kind in range(T + 1):
        if kind == T or p.main:
            for step in range(1, N):
                for copy in start(kind, partner(me, step, N)):
                    copy.wait_send()
    summed = []
    for q in range(RADIX):
        value = share[here, q]
        for hop in range(1, p.parts):
            across(hop, q).wait()
            value = value + shared[hop - 1, q]
        summed.append(value)
    lane = iota((rows, 128), 1)
    for tile in range(F // 128):
        begin = tile * 128 // RADIX
        block = begin // 128 * 128
        index = lane // RADIX + (begin - block)
        value = None
        for q in range(RADIX):
            picked = jnp.take_along_axis(summed[q][:, block : block + 128], index, axis=1)
            value = picked if value is None else jnp.where(lax.rem(lane, RADIX) == q, picked, value)
        out[:, tile * 128 : (tile + 1) * 128] = value


def per_device(visibility_real, visibility_imag, weights, labels, owner_of):
    row_count, times, channels = visibility_real.shape
    owners, parts = lax.axis_size("bl"), lax.axis_size("tm")
    p = Plan(row_count, times, channels, owner_of.shape[0], owners, parts)
    short = channels // RADIX
    inside = pl.BlockSpec(memory_space=pltpu.VMEM)
    outside = pl.BlockSpec(memory_space=pltpu.HBM)
    some = lambda count: max(count, 8)
    main, tail = some(p.main), some(p.tail)
    rows = p.per_owner // parts
    cut = 1 if owners & (owners - 1) else 2
    return pl.pallas_call(
        functools.partial(program_kernel, p),
        out_shape=pltpu.VMEM((rows, channels), F32),
        in_specs=[outside] * 5,
        out_specs=inside,
        scratch_shapes=[
            pltpu.VMEM((times, row_count), I32),
            pltpu.VMEM((row_count // 128, 128), I32),
            pltpu.VMEM((1, p.groups), I32),
            pltpu.VMEM((times // 2, 2, row_count, 2, channels), BF16),
            pltpu.VMEM((times // 2, 2, some(2 * p.mains), channels), F32),
            pltpu.VMEM((2, some(p.tails), channels), F32),
            pltpu.VMEM((times, owners, main, channels), I32),
            pltpu.VMEM((owners, tail, channels), I32),
            pltpu.VMEM((owners, 2, 128), F32),
            pltpu.VMEM((times, owners, main, channels), I32),
            pltpu.VMEM((owners, tail, channels), I32),
            pltpu.VMEM((owners, 2, 128), F32),
            pltpu.VMEM((RADIX, 2, short, 2 * short), BF16),
            pltpu.VMEM((1, channels), F32),
            pltpu.VMEM((2, times * p.per_owner, channels), F32),
            pltpu.VMEM((cut, 2, some(2 * p.mains) // cut, channels), BF16),
            pltpu.VMEM((times, RADIX, p.per_owner, 2 * short), F32),
            pltpu.VMEM((RADIX, p.per_owner, 2 * short), F32),
            pltpu.VMEM((parts, RADIX, rows, short), F32),
            pltpu.VMEM((parts - 1, RADIX, rows, short), F32),
            pltpu.SemaphoreType.DMA((times // 2, 2)),
            pltpu.SemaphoreType.DMA((3,)),
            pltpu.SemaphoreType.DMA((times + 2, owners)),
            pltpu.SemaphoreType.DMA((times + 2, owners)),
            pltpu.SemaphoreType.DMA((2,)),
            pltpu.SemaphoreType.DMA((parts - 1, RADIX)),
            pltpu.SemaphoreType.DMA((parts - 1, RADIX)),
        ],
        compiler_params=pltpu.CompilerParams(
            collective_id=0, has_side_effects=True, vmem_limit_bytes=60 * 2**20
        ),
    )(visibility_real, visibility_imag, weights.T, labels.reshape(-1, 128), owner_of[None, :])


def solution(mesh):
    placed = (P("bl", "tm", None), P("bl", "tm", None), P("bl", "tm"), P("bl"), P())
    return jax.shard_map(
        per_device, mesh=mesh, in_specs=placed, out_specs=P(("bl", "tm"), None), check_vma=False
    )
```

```python
import functools
import math

import jax
import jax.numpy as jnp
from jax import lax
from jax.experimental import pallas as pl
from jax.experimental.pallas import tpu as pltpu
from jax.sharding import PartitionSpec as P

HARRIS = (0.35875, 0.48829, 0.14128, 0.01168)
RADIX = 4
F32, BF16, I32 = jnp.float32, jnp.bfloat16, jnp.int32
MESH = pl.DeviceIdType.MESH


def iota(shape, dim):
    return lax.broadcasted_iota(I32, shape, dim)


def dot(a, b):
    return jnp.dot(a, b, preferred_element_type=F32)


def halves(value):
    high = value.astype(BF16)
    return high, (value - high.astype(F32)).astype(BF16)


def lanes(count):
    return -(-max(count, 1) // 128) * 128


def partner(me, step, size):
    if size & (size - 1):
        return lax.rem(me + step, size)
    peer, bit = 0, 1
    while bit < size:
        peer = peer + bit * lax.rem(lax.rem(me // bit, 2) + step // bit, 2)
        bit *= 2
    return peer


class Plan:
    def __init__(self, row_count, times, channels, groups, owners, parts):
        capacity = 3 * row_count // (2 * owners)
        self.rows, self.times, self.channels, self.groups = row_count, times, channels, groups
        self.owners, self.parts = owners, parts
        self.per_owner = groups // owners
        self.distinct = min(capacity // 4, self.per_owner // 2)
        self.main = self.distinct // 16 * 16
        self.extra = self.distinct - self.main
        self.tail = -(-self.extra * times // 8) * 8
        self.mains = owners * self.main
        self.tails = owners * self.tail
        assert times * self.main + self.tail <= 128


def program_kernel(
    plan, vis_real, vis_imag, weights, labels, owner_of, out,
    weight_in, label_in, owner_in,
    fresh, part, part_tail, send, send_tail, send_note,
    came, came_tail, came_note,
    table, taper, total, planes, spectrum, following, share, shared,
    loads, small, sends, arrivals, ahead_sems, tail_sends, tail_arrivals,
):
    p = plan
    T, N, F, G, R = p.times, p.owners, p.channels, p.groups, p.rows
    pairs, both = T // 2, 2 * R
    short = F // RADIX
    n = p.per_owner
    me = lax.axis_index("bl")
    here = lax.axis_index("tm")

    inputs = [
        pltpu.make_async_copy(source, target, small.at[index])
        for index, (source, target) in enumerate(
            ((labels, label_in), (weights, weight_in), (owner_of, owner_in))
        )
    ]
    for copy in inputs:
        copy.start()
    incoming = []
    for pair in range(pairs):
        for which, source in enumerate((vis_real, vis_imag)):
            copy = pltpu.make_async_copy(
                source.at[:, pl.ds(2 * pair, 2)], fresh.at[pair, which], loads.at[pair, which]
            )
            incoming.append(copy)
    for copy in incoming[:2]:
        copy.start()

    barrier = pltpu.get_barrier_semaphore()
    for hop in range(1, N):
        pl.semaphore_signal(
            barrier, inc=1, device_id={"bl": lax.rem(me + hop, N)}, device_id_type=MESH
        )
    for hop in range(1, p.parts):
        pl.semaphore_signal(
            barrier, inc=1, device_id={"tm": lax.rem(here + hop, p.parts)}, device_id_type=MESH
        )

    spread = (iota((R, both), 1) // 2 == iota((R, both), 0)).astype(F32).astype(BF16)
    before = (iota((G, G), 0) < iota((G, G), 1)).astype(F32).astype(BF16)
    for copy in inputs:
        copy.wait()
    label = jnp.concatenate(
        [label_in[i : i + 1] for i in range(label_in.shape[0])], axis=1
    )
    hit = (iota((G, R), 0) == label).astype(F32).astype(BF16)
    count = lax.dot_general(
        jnp.ones((8, R), BF16), hit, (((1,), (1,)), ((), ())), preferred_element_type=F32
    )
    present = (count[0:1] > 0.5).astype(F32)
    owner = owner_in[...]
    owned = (iota((N, G), 0) == owner).astype(F32)
    earlier = dot(jnp.concatenate([owned, owned * present], axis=0).astype(BF16), before)
    rank = jnp.sum(owned * earlier[:N], axis=0, keepdims=True)
    order = jnp.sum(owned * earlier[N:], axis=0, keepdims=True)
    info = jnp.concatenate([owner.astype(F32), order, jnp.zeros((6, G), F32)], axis=0)
    placed = dot(info.astype(BF16), hit)[:2]
    base = jnp.concatenate(
        [placed, weight_in[...].astype(F32), jnp.zeros((-(T + 2) % 8, R), F32)], axis=0
    )
    doubled = dot(base.astype(BF16), spread)
    row_owner = doubled[0:1].astype(I32)
    row_order = doubled[1:2].astype(I32)
    second = lax.rem(iota((1, both), 1), 2)

    def ranks():
        listed = order.astype(I32)
        seen = present > 0.5
        rank_main = rank_tail = None
        if p.main:
            slot_main = jnp.where(seen & (listed < p.main), owner * p.main + listed, -1)
            rank_main = jnp.sum(
                jnp.where(iota((p.mains, G), 0) == slot_main, rank, 0.0), axis=1, keepdims=True
            )
        if p.extra:
            slot_tail = jnp.where(
                seen & (listed >= p.main), owner * p.extra + listed - p.main, -1
            )
            row = iota((p.tails, 1), 0)
            within = lax.rem(row, p.tail)
            slot_of_row = row // p.tail * p.extra + lax.rem(within, p.extra)
            rank_tail = jnp.sum(
                jnp.where((slot_of_row == slot_tail) & (within < p.extra * T), rank, 0.0),
                axis=1,
                keepdims=True,
            )
        return rank_main, rank_tail

    def laid(column, height, offset):
        shape = (column.shape[0], 128)
        match = lax.rem(iota(shape, 0), height) == iota(shape, 1) - offset
        block = jnp.where(match, jnp.broadcast_to(column, shape), 0.0)
        return jnp.sum(block.reshape(shape[0] // height, height, 128), axis=1, keepdims=True)

    base_tail = T * p.main
    note = jnp.zeros((N, 1, 128), F32)
    send_note[...] = jnp.zeros_like(send_note)

    def start(kind, peer):
        if kind < T:
            pieces = [(send.at[kind], came.at[kind], kind)]
        else:
            pieces = [(send_note, came_note, T + 1)]
            if p.extra:
                pieces.append((send_tail, came_tail, T))
        return [
            pltpu.make_async_remote_copy(
                src_ref=source.at[peer],
                dst_ref=target.at[me],
                send_sem=sends.at[index, peer],
                recv_sem=arrivals.at[index, me],
                device_id={"bl": peer},
                device_id_type=MESH,
            )
            for source, target, index in pieces
        ]

    def arrive(kind, source):
        if kind < T:
            pieces = [(send.at[kind], came.at[kind], kind)]
        else:
            pieces = [(send_note, came_note, T + 1)]
            if p.extra:
                pieces.append((send_tail, came_tail, T))
        return [
            pltpu.make_async_remote_copy(
                src_ref=origin.at[source],
                dst_ref=target.at[source],
                send_sem=sends.at[index, source],
                recv_sem=arrivals.at[index, source],
                device_id={"bl": source},
                device_id_type=MESH,
            )
            for origin, target, index in pieces
        ]

    def post(kind, peer):
        for copy in start(kind, peer):
            copy.start()

    def encode(real, imag):
        peak = jnp.maximum(
            jnp.max(jnp.abs(real), axis=1, keepdims=True),
            jnp.max(jnp.abs(imag), axis=1, keepdims=True),
        )
        step = jnp.maximum(peak, 1e-30) * (1.0078125 / 32767.0)
        step = step.astype(BF16).astype(F32)
        invert = 1.0 / step
        code_real = jnp.round(real * invert).astype(I32)
        code_imag = jnp.round(imag * invert).astype(I32)
        return (code_real << 16) | (code_imag & 65535), step

    def encode_main(time, o):
        at = pl.multiple_of(time % 2 * p.mains + o * p.main, 16)
        rows = pl.ds(at, p.main)
        code, step = encode(part[time // 2, 0, rows], part[time // 2, 1, rows])
        send_note[o, 1:2] += laid(step, p.main, time * p.main)[0]
        return code

    def encode_tail(o):
        rows = pl.ds(pl.multiple_of(o * p.tail, 8), p.tail)
        code, step = encode(part_tail[0, rows], part_tail[1, rows])
        send_note[o, 1:2] += laid(step, p.tail, base_tail)[0]
        return code

    def handle_main(time, now):
        def one(step, carry):
            peer = partner(me, step, N)
            send[time, peer] = encode_main(time, peer)
            if now:
                post(time, peer)
            return carry

        if now:
            lax.fori_loop(N // 2, N, lambda i, c: one(N + N // 2 - 1 - i, c), 0)
            lax.fori_loop(1, N // 2, one, 0)
        else:
            lax.fori_loop(1, N, one, 0)
        came[time, me] = encode_main(time, me)

    def handle_tail():
        def one(step, carry):
            peer = partner(me, step, N)
            send_tail[peer] = encode_tail(peer)
            return carry

        lax.fori_loop(1, N, one, 0)
        came_tail[me] = encode_tail(me)

    all_rows = 2 * p.mains + p.tails
    tail_weight = jnp.zeros((p.tails, 1), F32)
    for pair in range(pairs):
        weight = jnp.where(
            second == 0, doubled[2 + 2 * pair : 3 + 2 * pair], doubled[3 + 2 * pair : 4 + 2 * pair]
        )
        target = jnp.where(
            row_order < p.main,
            second * p.mains + row_owner * p.main + row_order,
            2 * p.mains
            + row_owner * p.tail
            + (2 * pair + second) * p.extra
            + row_order
            - p.main,
        )
        folder = jnp.where(iota((all_rows, both), 0) == target, weight, 0.0)
        full, folder = folder, folder.astype(BF16)
        for copy in incoming[2 * pair : 2 * pair + 2]:
            copy.wait()
        for copy in incoming[2 * pair + 2 : 2 * pair + 4]:
            copy.start()
        bounds = [0, all_rows]
        if pair == 0 and p.main:
            bounds = [0, p.mains, all_rows]
        for low, high in zip(bounds, bounds[1:]):
            for which in range(2):
                made = dot(folder[low:high], fresh[pair, which].reshape(both, F))
                middle = max(2 * p.mains - low, 0)
                if middle:
                    part[pair, which, low : min(high, 2 * p.mains)] = made[:middle]
                if p.extra and high == all_rows:
                    if pair:
                        part_tail[which] += made[middle:]
                    else:
                        part_tail[which] = made[middle:]
            if pair == 0 and low == 0:
                pl.semaphore_wait(barrier, N + p.parts - 2)
                if p.main:
                    handle_main(0, True)
        sums = jnp.sum(full, axis=1, keepdims=True)
        if pair == 0:
            rank_main, rank_tail = ranks()
        if p.main:
            for which in range(2):
                fact = sums[which * p.mains : (which + 1) * p.mains] * n + rank_main
                note = note + laid(fact, p.main, (2 * pair + which) * p.main)
        if p.extra:
            tail_weight = tail_weight + sums[2 * p.mains :]
        if p.main:
            for time in range(max(2 * pair, 1), 2 * pair + 2):
                handle_main(time, False)
    if p.extra:
        note = note + laid(tail_weight * n + rank_tail, p.tail, base_tail)
        handle_tail()
    send_note[:, 0:1] = note
    came_note[me] = send_note[me]
    for kind in [T] + list(range(1, T if p.main else 1)):
        for step in range(1, N):
            post(kind, partner(me, step, N))

    turn = 2.0 * math.pi / F
    phase = turn * iota((1, F), 1).astype(F32)
    shape = (
        HARRIS[0]
        - HARRIS[1] * jnp.cos(phase)
        + HARRIS[2] * jnp.cos(2.0 * phase)
        - HARRIS[3] * jnp.cos(3.0 * phase)
    )
    taper[...] = shape / jnp.sqrt(jnp.sum(shape * shape, axis=1, keepdims=True))
    fine = 16
    for q in range(RADIX):
        delay = RADIX * iota((fine, short), 1) + q
        low = turn * lax.rem(iota((fine, short), 0) * delay, F).astype(F32)
        high = turn * lax.rem(fine * iota((fine, short), 0) * delay, F).astype(F32)
        low_cos, low_sin = jnp.cos(low), jnp.sin(low)
        high_cos, high_sin = jnp.cos(high), jnp.sin(high)
        for a in range(short // fine):
            ac, as_ = high_cos[a : a + 1], high_sin[a : a + 1]
            rows = pl.ds(a * fine, fine)
            upper, lower = halves(ac * low_cos - as_ * low_sin)
            table[q, 0, rows, :short] = upper
            table[q, 1, rows, :short] = lower
            upper, lower = halves(as_ * low_cos + ac * low_sin)
            table[q, 0, rows, short:] = upper
            table[q, 1, rows, short:] = lower

    def wait_for(kind, source):
        for copy in arrive(kind, source):
            copy.wait_recv()

    cut = 1 if N & (N - 1) else 2
    group = N // cut
    mine = me // group

    def split(code):
        imag = (code << 16) >> 16
        parts = (code >> 24, (code >> 16) & 255, imag >> 8, imag & 255)
        return [part.astype(F32).astype(BF16) for part in parts]

    def gathered(values, height, offset):
        values = values.reshape(N, 128)
        blocks = []
        for block in range(lanes(N * height) // 128):
            lane = iota((N, 128), 1) + block * 128
            picked = jnp.take_along_axis(values, offset + lax.rem(lane, height), axis=1)
            mine = lane // height == iota((N, 128), 0)
            blocks.append(jnp.sum(jnp.where(mine, picked, 0.0), axis=0, keepdims=True))
        return jnp.concatenate(blocks, axis=1)[:, : N * height]

    def facts_of(values, height, offset):
        fact = gathered(values, height, offset).astype(I32)
        return lax.rem(fact, n), (fact // n).astype(F32)

    for step in range(1, N):
        wait_for(T, partner(me, step, N))
    facts, steps = came_note[:, 0], came_note[:, 1]
    rank_row = iota((n, 1), 0)
    main_picks = []
    if p.main:
        for time in range(T):
            rank, heft = facts_of(facts, p.main, time * p.main)
            chosen = rank_row == rank
            heft = jnp.sum(jnp.where(chosen, heft, 0.0), axis=1, keepdims=True)
            selector = jnp.where(chosen, gathered(steps, p.main, time * p.main), 0.0)
            main_picks.append((selector, heft))
    tail_sums = []
    if p.extra:
        tail_rank, tail_heft = facts_of(facts, p.tail, base_tail)
        tail_step = gathered(steps, p.tail, base_tail)
        pieces = split(came_tail[...].reshape(p.tails, F))
        lane = lax.rem(iota((1, p.tails), 1), p.tail)
        lane_time = jnp.where(lane < p.extra * T, lane // p.extra, T)
        selectors = []
        for time in range(T):
            chosen = (rank_row == tail_rank) & (lane_time == time)
            selector = jnp.where(chosen, tail_step, 0.0)
            selectors.append(jnp.concatenate([256.0 * selector, selector], axis=1))
            tail_sums.append(jnp.sum(jnp.where(chosen, tail_heft, 0.0), axis=1, keepdims=True))
        selectors = jnp.concatenate(selectors, axis=0).astype(BF16)
        total[0] = dot(selectors, jnp.concatenate(pieces[:2], axis=0))
        total[1] = dot(selectors, jnp.concatenate(pieces[2:], axis=0))

    ahead = pltpu.make_async_remote_copy(
        src_ref=spectrum.at[0],
        dst_ref=following,
        send_sem=ahead_sems.at[0],
        recv_sem=ahead_sems.at[1],
        device_id={"tm": lax.rem(here + p.parts - 1, p.parts)},
        device_id_type=MESH,
    )
    rows = n // p.parts

    def across(hop, q):
        return pltpu.make_async_remote_copy(
            src_ref=share.at[lax.rem(here + hop, p.parts), q],
            dst_ref=shared.at[hop - 1, q],
            send_sem=tail_sends.at[hop - 1, q],
            recv_sem=tail_arrivals.at[hop - 1, q],
            device_id={"tm": lax.rem(here + hop, p.parts)},
            device_id_type=MESH,
        )

    def power_of(product):
        return (product[:, :short] + product[:, short:]).reshape(p.parts, rows, short)

    for time in range(T):
        weight_sum = jnp.zeros((n, 1), F32)
        if p.extra:
            weight_sum = weight_sum + tail_sums[time]
        if p.main:

            selector_all, heft = main_picks[time]
            weight_sum = weight_sum + heft
            real = imag = 0.0
            if p.extra:
                block = pl.ds(time * n, n)
                real, imag = total[0, block], total[1, block]
            wide = group * p.main
            for near in range(cut):
                members = range(near * group, (near + 1) * group)
                for step in members:
                    source = partner(me, step, N) if step else me
                    if step:
                        wait_for(time, source)
                    for which, piece in enumerate(split(came[time, source])):
                        at = which % 2 * wide + lax.rem(source, group) * p.main
                        at = pl.ds(pl.multiple_of(at, 16), p.main)
                        planes[near, which // 2, at] = piece
                selector = selector_all
                if cut == 2:
                    selector = jnp.where(
                        (mine + near) % 2 == 0, selector[:, :wide], selector[:, wide:]
                    )
                selector = jnp.concatenate([256.0 * selector, selector], axis=1).astype(BF16)
                real = real + dot(selector, planes[near, 0])
                imag = imag + dot(selector, planes[near, 1])
        else:
            block = pl.ds(time * n, n)
            real, imag = total[0, block], total[1, block]
        scale = 1.0 / jnp.maximum(weight_sum, 1.0)
        window = taper[...]
        real = real * scale * window
        imag = imag * scale * window
        r = [real[:, i * short : (i + 1) * short] for i in range(RADIX)]
        m = [imag[:, i * short : (i + 1) * short] for i in range(RADIX)]
        er, ei, fr, fi = r[0] + r[2], m[0] + m[2], r[1] + r[3], m[1] + m[3]
        gr, gi, hr, hi = r[0] - r[2], m[0] - m[2], r[1] - r[3], m[1] - m[3]
        folded = (
            (er + fr, ei + fi),
            (gr + hi, gi - hr),
            (er - fr, ei - fi),
            (gr - hi, gi + hr),
        )
        if time == T - 1:
            ahead.wait()
        for q in range(RADIX):
            upper, lower = halves(jnp.concatenate(folded[q], axis=0))
            first = dot(jnp.concatenate([upper, lower], axis=0), table[q, 0])
            wave = first[: 2 * n] + first[2 * n :] + dot(upper, table[q, 1])
            now = jnp.concatenate(
                [wave[:n, :short] + wave[n:, short:], wave[n:, :short] - wave[:n, short:]],
                axis=1,
            )
            spectrum[time, q] = now
            if time:
                power = power_of(spectrum[time - 1, q] * now)
                if time > 1:
                    power = power + share[:, q]
                if time == T - 1:
                    beyond = power_of(now * following[q])
                    power = power + jnp.where(here < p.parts - 1, beyond, 0.0)
                share[:, q] = power
                if time == T - 1 and q % 2 == 1:
                    for part_q in range(q - 1, q + 1):
                        for hop in range(1, p.parts):
                            across(hop, part_q).start()
        if time == 0:
            ahead.start()

    for kind in range(T + 1):
        if kind == T or p.main:
            for step in range(1, N):
                for copy in start(kind, partner(me, step, N)):
                    copy.wait_send()
    summed = []
    for q in range(RADIX):
        value = share[here, q]
        for hop in range(1, p.parts):
            across(hop, q).wait()
            value = value + shared[hop - 1, q]
        summed.append(value)
    lane = iota((rows, 128), 1)
    for tile in range(F // 128):
        begin = tile * 128 // RADIX
        block = begin // 128 * 128
        index = lane // RADIX + (begin - block)
        value = None
        for q in range(RADIX):
            picked = jnp.take_along_axis(summed[q][:, block : block + 128], index, axis=1)
            value = picked if value is None else jnp.where(lax.rem(lane, RADIX) == q, picked, value)
        out[:, tile * 128 : (tile + 1) * 128] = value


def per_device(visibility_real, visibility_imag, weights, labels, owner_of):
    row_count, times, channels = visibility_real.shape
    owners, parts = lax.axis_size("bl"), lax.axis_size("tm")
    p = Plan(row_count, times, channels, owner_of.shape[0], owners, parts)
    short = channels // RADIX
    inside = pl.BlockSpec(memory_space=pltpu.VMEM)
    outside = pl.BlockSpec(memory_space=pltpu.HBM)
    some = lambda count: max(count, 8)
    main, tail = some(p.main), some(p.tail)
    rows = p.per_owner // parts
    cut = 1 if owners & (owners - 1) else 2
    return pl.pallas_call(
        functools.partial(program_kernel, p),
        out_shape=pltpu.VMEM((rows, channels), F32),
        in_specs=[outside] * 5,
        out_specs=inside,
        scratch_shapes=[
            pltpu.VMEM((times, row_count), I32),
            pltpu.VMEM((row_count // 128, 128), I32),
            pltpu.VMEM((1, p.groups), I32),
            pltpu.VMEM((times // 2, 2, row_count, 2, channels), BF16),
            pltpu.VMEM((times // 2, 2, some(2 * p.mains), channels), F32),
            pltpu.VMEM((2, some(p.tails), channels), F32),
            pltpu.VMEM((times, owners, main, channels), I32),
            pltpu.VMEM((owners, tail, channels), I32),
            pltpu.VMEM((owners, 2, 128), F32),
            pltpu.VMEM((times, owners, main, channels), I32),
            pltpu.VMEM((owners, tail, channels), I32),
            pltpu.VMEM((owners, 2, 128), F32),
            pltpu.VMEM((RADIX, 2, short, 2 * short), BF16),
            pltpu.VMEM((1, channels), F32),
            pltpu.VMEM((2, times * p.per_owner, channels), F32),
            pltpu.VMEM((cut, 2, some(2 * p.mains) // cut, channels), BF16),
            pltpu.VMEM((times, RADIX, p.per_owner, 2 * short), F32),
            pltpu.VMEM((RADIX, p.per_owner, 2 * short), F32),
            pltpu.VMEM((parts, RADIX, rows, short), F32),
            pltpu.VMEM((parts - 1, RADIX, rows, short), F32),
            pltpu.SemaphoreType.DMA((times // 2, 2)),
            pltpu.SemaphoreType.DMA((3,)),
            pltpu.SemaphoreType.DMA((times + 2, owners)),
            pltpu.SemaphoreType.DMA((times + 2, owners)),
            pltpu.SemaphoreType.DMA((2,)),
            pltpu.SemaphoreType.DMA((parts - 1, RADIX)),
            pltpu.SemaphoreType.DMA((parts - 1, RADIX)),
        ],
        compiler_params=pltpu.CompilerParams(
            collective_id=0, has_side_effects=True, vmem_limit_bytes=60 * 2**20
        ),
    )(visibility_real, visibility_imag, weights.T, labels.reshape(-1, 128), owner_of[None, :])


def solution(mesh):
    placed = (P("bl", "tm", None), P("bl", "tm", None), P("bl", "tm"), P("bl"), P())
    return jax.shard_map(
        per_device, mesh=mesh, in_specs=placed, out_specs=P(("bl", "tm"), None), check_vma=False
    )
```
